32 devices in a mesh: elem: 8 (over z, y), comp: 2 (over x), rep: 2 (over core).
Axes of the slice: x: 2, y: 2, z: 4, core: 2. Of those that a mesh axis runs over, the one named last changes fastest.
Arguments:
- velocity: float32 [3, 10, 10, 10, 2, 6144], P(None, 'comp', None, None, None, ('elem', 'rep')), may hold values from -6 to 6
- geometry: float32 [3, 3, 10, 10, 10, 2, 6144], P(None, None, 'comp', None, None, None, ('elem', 'rep')), may hold values from -40 to 40
- element_place: int32 [2, 6144], P('comp', ('elem', 'rep')), may hold values from 0 to 383, as said below
Outputs:
- pressure: float32 [10, 10, 10, 2, 6144], P(None, None, None, 'comp', ('elem', 'rep'))
The draws below stay inside these ranges and needn't reach their ends.
Inputs may be any that keep to these rules, and one draw needn't show every extreme that they name: `element_place`: in each row and each aligned run of 384 entries of it, every value 0 to 383 appears once.
All inputs are finite; a program needn't handle non-finite values.
Results may differ from the reference program's by a relative error of at most 0.000071.
Values sent between devices are 32-bit elements; how exact they have to be, the bound alone decides.
A program may use at most 192 MiB of HBM per device.

```python
import jax
import jax.numpy as jnp
import numpy as np
from jax import lax

NODES = 10
BLOCK_X = 6
BLOCK_Y = 8
BLOCK_Z = 8
GRID_Y = 4
SUB_ELEMS = 384
ROW_ELEMS = 6144
BOX_X = 12
BOX_Y = 32
BOX_Z = 32
N_COMP = 2
N_REP = 2


def draw_geometry(key, part):
    base_key = jax.random.fold_in(key, 31)
    weight_key, mixing_key = jax.random.split(base_key)
    node_shape = (NODES, NODES, NODES, N_COMP, ROW_ELEMS)
    full_shape = (3, 3) + node_shape
    weights = jax.random.uniform(weight_key, node_shape, jnp.float32, 0.5, 2.0)
    mixing = 0.35 * jax.random.truncated_normal(mixing_key, -4.0, 4.0, full_shape, jnp.float32)
    mixing = mixing + jnp.eye(3, dtype=jnp.float32).reshape(3, 3, 1, 1, 1, 1, 1)
    return (weights[None, None] * mixing).astype(jnp.float32)


def draw_element_place(key, part):
    blocks = N_COMP * ROW_ELEMS // SUB_ELEMS
    block_keys = jax.random.split(jax.random.fold_in(key, 7), blocks)

    def one_order(block_key):
        return jax.random.permutation(block_key, SUB_ELEMS)
    orders = jax.vmap(one_order)(block_keys)
    return orders.reshape(N_COMP, ROW_ELEMS).astype(jnp.int32)


def steps_of(key, shape, pieces, smallest, top_value):
    gain, own = 1.0, jax.random.fold_in(key, 6)
    for axis_at, blocks in pieces:
        draws = jnp.exp(jax.random.uniform(jax.random.fold_in(own, axis_at), (blocks,), jnp.float32, smallest / len(pieces), top_value / len(pieces)))
        gain = gain * jnp.repeat(draws, shape[axis_at] // blocks).reshape([-1 if axis == axis_at else 1 for axis in range(len(shape))])
    return gain


def scatter_about(rng, shape, scale, most, cuts=(), held_as=jnp.bfloat16):
    drawn = jax.random.normal(rng, shape, jnp.float32) * scale
    if len(cuts) > 0:
        drawn = steps_of(rng, shape, cuts, -0.22, 0.18) * drawn
    return jnp.clip(drawn, min=-most, max=most).astype(held_as)


def setup_inputs(seed: int = 0) -> dict:
    key_of = jax.random.split(jax.random.key(seed), 4)
    return {
        "velocity": scatter_about(key_of[0], (3, NODES, NODES, NODES, N_COMP, ROW_ELEMS), 1.0, 6.0, ((1, 2), (5, 16)), jnp.float32),
        "geometry": draw_geometry(jax.random.fold_in(key_of[3], 71), 0),
        "element_place": draw_element_place(jax.random.fold_in(key_of[3], 71), 0),
    }


exact_mode = lax.Precision.HIGHEST


def legendre_columns(points, degree):
    columns = [points * 0.0 + 1.0, points]
    for order in range(2, degree + 1):
        columns.append(((2 * order - 1) * points * columns[order - 1] - (order - 1) * columns[order - 2]) / order)
    return columns


def derivative_table(node_count):
    degree = node_count - 1
    points = np.cos(np.pi * np.arange(node_count) / degree)
    for sweep in range(100):
        columns = legendre_columns(points, degree)
        points = points - (points * columns[degree] - columns[degree - 1]) / (node_count * columns[degree])
    points = np.sort(points)
    values = legendre_columns(points, degree)[degree]
    identity = np.eye(node_count)
    spacing = points[:, None] - points[None, :] + identity
    matrix = values[:, None] / (values[None, :] * spacing)
    matrix = np.where(identity > 0.5, 0.0, matrix)
    matrix[0, 0] = -degree * (degree + 1) / 4.0
    matrix[degree, degree] = degree * (degree + 1) / 4.0
    return matrix


def apply_transpose(deriv_table, flux_r, flux_s, flux_t):
    along_r = jnp.einsum("ia,i...->a...", deriv_table, flux_r, precision=exact_mode)
    along_s = jnp.einsum("ib,ai...->ab...", deriv_table, flux_s, precision=exact_mode)
    along_t = jnp.einsum("ic,abi...->abc...", deriv_table, flux_t, precision=exact_mode)
    return along_r + along_s + along_t


def local_pass(field, direction, block_grid):
    last_node = field.shape[0] - 1
    low_key = tuple(0 if dim_index == direction else slice(None) for dim_index in range(3))
    high_key = tuple(last_node if dim_index == direction else slice(None) for dim_index in range(3))
    lower = field[low_key]
    upper = field[high_key]
    leading = lower.shape[:-1]
    lower = lower.reshape(leading + tuple(block_grid))
    upper = upper.reshape(leading + tuple(block_grid))
    element_axis = len(leading) + direction
    extent = block_grid[direction]
    summed = lax.slice_in_dim(upper, 0, extent - 1, axis=element_axis) + lax.slice_in_dim(lower, 1, extent, axis=element_axis)
    upper = jnp.concatenate([summed, lax.slice_in_dim(upper, extent - 1, extent, axis=element_axis)], axis=element_axis)
    lower = jnp.concatenate([lax.slice_in_dim(lower, 0, 1, axis=element_axis), summed], axis=element_axis)
    field = field.at[low_key].set(lower.reshape(leading + (-1,)))
    return field.at[high_key].set(upper.reshape(leading + (-1,)))


def element_cells(element_place):
    row_index = jnp.arange(ROW_ELEMS, dtype=jnp.int32)[None, :]
    half_index = jnp.arange(N_COMP, dtype=jnp.int32)[:, None]
    block_index = row_index // SUB_ELEMS
    layers = N_COMP * N_REP
    sub_block = (block_index // N_REP) * layers + half_index * N_REP + block_index % N_REP
    cell_x = (sub_block // (GRID_Y * layers)) * BLOCK_X + element_place // (BLOCK_Y * BLOCK_Z)
    cell_y = ((sub_block // layers) % GRID_Y) * BLOCK_Y + (element_place // BLOCK_Z) % BLOCK_Y
    cell_z = (sub_block % layers) * BLOCK_Z + element_place % BLOCK_Z
    return ((cell_x * BOX_Y + cell_y) * BOX_Z + cell_z).astype(jnp.int32)


def reference(velocity, geometry, element_place):
    deriv_table = jnp.asarray(derivative_table(NODES), jnp.float32)
    fluxes = []
    for direction in range(3):
        fluxes.append(geometry[0, direction] * velocity[0] + geometry[1, direction] * velocity[1] + geometry[2, direction] * velocity[2])
    local_div = apply_transpose(deriv_table, fluxes[0], fluxes[1], fluxes[2])
    flat_cells = element_cells(element_place).reshape(-1).astype(jnp.int32)
    flat_local = local_div.reshape(NODES, NODES, NODES, N_COMP * ROW_ELEMS)
    box_field = jnp.zeros((NODES, NODES, NODES, BOX_X * BOX_Y * BOX_Z), jnp.float32)
    box_field = box_field.at[:, :, :, flat_cells].set(flat_local)
    for direction in range(3):
        box_field = local_pass(box_field, direction, (BOX_X, BOX_Y, BOX_Z))
    pressure = box_field[:, :, :, flat_cells]
    return pressure.reshape(NODES, NODES, NODES, N_COMP, ROW_ELEMS)
```

```python
import functools

import jax
import jax.numpy as jnp
import numpy as np
from jax import lax
from jax.experimental import pallas as pl
from jax.experimental.pallas import tpu as pltpu
from jax.sharding import PartitionSpec as P

BLOCK = (6, 8, 8)
GRID_Y = 4
LANES = 128
MESH = pl.DeviceIdType.MESH
AWAY = -100000


def legendre_columns(points, degree):
    columns = [points * 0.0 + 1.0, points]
    for order in range(2, degree + 1):
        columns.append(
            ((2 * order - 1) * points * columns[order - 1] - (order - 1) * columns[order - 2])
            / order
        )
    return columns


def derivative_table(node_count):
    degree = node_count - 1
    points = np.cos(np.pi * np.arange(node_count) / degree)
    for sweep in range(100):
        columns = legendre_columns(points, degree)
        points = points - (points * columns[degree] - columns[degree - 1]) / (
            node_count * columns[degree]
        )
    points = np.sort(points)
    values = legendre_columns(points, degree)[degree]
    identity = np.eye(node_count)
    spacing = points[:, None] - points[None, :] + identity
    matrix = values[:, None] / (values[None, :] * spacing)
    matrix = np.where(identity > 0.5, 0.0, matrix)
    matrix[0, 0] = -degree * (degree + 1) / 4.0
    matrix[degree, degree] = degree * (degree + 1) / 4.0
    return matrix


def up(count, step):
    return -(-count // step) * step


class Rows:
    def __init__(self, n):
        self.n = n
        m = n - 2
        self.m = m
        self.c_low, self.c_high = 0, m
        self.b_low, self.b_high = 2 * m, 2 * m + n
        self.faces = up(2 * m + 2 * n, 8)
        self.plane = n * n
        self.plane_pad = up(n * n, 8)
        self.total = self.faces + m * m

    def nodes(self):
        n, m = self.n, self.m
        order = [None] * up(self.total, 8)
        for k in range(m):
            order[self.c_low + k] = (k + 1, 0)
            order[self.c_high + k] = (k + 1, n - 1)
        for k in range(n):
            order[self.b_low + k] = (0, k)
            order[self.b_high + k] = (n - 1, k)
        for b in range(m):
            for c in range(m):
                order[self.faces + b * m + c] = (b + 1, c + 1)
        return order


def plane_matrix(table, rows):
    n = rows.n
    order = rows.nodes()
    matrix = np.zeros((len(order), 2 * rows.plane_pad), np.float32)
    for r, node in enumerate(order):
        if node is not None:
            b, c = node
            for i in range(n):
                matrix[r, i * n + c] += table[i, b]
                matrix[r, rows.plane_pad + b * n + i] += table[i, c]
    top = jnp.asarray(matrix).astype(jnp.bfloat16)
    rest = (jnp.asarray(matrix) - top.astype(jnp.float32)).astype(jnp.bfloat16)
    return jnp.concatenate([top, rest], axis=0)


def halves(x):
    high = x.astype(jnp.bfloat16)
    low = (x - high.astype(jnp.float32)).astype(jnp.bfloat16)
    return high, low


def dot(a, b):
    return jnp.dot(a, b, preferred_element_type=jnp.float32)


def pair_dot(x, onehot):
    high, low = halves(x)
    return dot(high, onehot) + dot(low, onehot)


def kernel(sizes, place_ref, kmat_ref, vel_ref, geo_ref, out_ref,
           vel, geo, flux, stack, fbuf, sbuf, field, face, near, sel, selt, outb, inb,
           load_sem, fsend, frecv, ssend, srecv, isend, irecv, nsend, nrecv):
    n, half, tiles, table, rows, counts = sizes
    m = rows.m
    parts = tiles * 2
    comp_count, rep_count = counts
    e, h, r = lax.axis_index("elem"), lax.axis_index("comp"), lax.axis_index("rep")
    elem_count = lax.axis_size("elem")
    other = 1 - h
    layers = comp_count * rep_count
    device = e * layers + h * rep_count + r
    stride_x = GRID_Y * layers
    extents = (elem_count * layers // stride_x, GRID_Y, layers)
    strides = (stride_x, layers, 1)
    position = (device // stride_x, (device // layers) % GRID_Y, device % layers)

    def coords(target):
        return (target // layers, (target // rep_count) % comp_count, target % rep_count)

    def has(d, side):
        if side == 0:
            return position[d] > 0
        return position[d] < extents[d] - 1

    def neighbour(d, side):
        return coords(device + (strides[d] if side == 1 else -strides[d]))

    def plane_at(k):
        return h * (half - 1) + k * (1 - 2 * h)

    def load(k, what):
        i = plane_at(k)
        if what == 0:
            return pltpu.make_async_copy(vel_ref.at[:, i], vel.at[:, i], load_sem.at[0, k])
        if what == 1:
            return pltpu.make_async_copy(geo_ref.at[:, 0, i], geo.at[:, 0, i], load_sem.at[1, k])
        return pltpu.make_async_copy(
            geo_ref.at[:, pl.ds(1, 2), i], geo.at[:, pl.ds(1, 2), i], load_sem.at[2, k]
        )

    for k in range(half):
        load(k, 0).start()
        load(k, 1).start()
    for k in range(half):
        load(k, 2).start()

    barrier = pltpu.get_barrier_semaphore()
    pl.semaphore_signal(barrier, inc=1, device_id=(e, other, r), device_id_type=MESH)
    expected = jnp.int32(1)
    for d in range(3):
        for side in range(2):
            @pl.when(has(d, side))
            def _():
                pl.semaphore_signal(
                    barrier, inc=1, device_id=neighbour(d, side), device_id_type=MESH
                )
            expected = expected + has(d, side).astype(jnp.int32)
    pl.semaphore_wait(barrier, expected)

    peer = (e, other, r)

    def flux_copy(k, first):
        a = first * half + (first * (half - 1) + k * (1 - 2 * first))
        q = 1 - first
        return pltpu.make_async_remote_copy(
            src_ref=fbuf.at[q, a], dst_ref=fbuf.at[q, a], send_sem=fsend.at[k],
            recv_sem=frecv.at[k], device_id=peer, device_id_type=MESH)

    def face_copy(k, first):
        a = first * half + (first * (half - 1) + k * (1 - 2 * first))
        q = 1 - first
        ref = sbuf.at[q, a, :, pl.ds(0, rows.faces)]
        return pltpu.make_async_remote_copy(
            src_ref=ref, dst_ref=ref, send_sem=ssend.at[k],
            recv_sem=srecv.at[k], device_id=peer, device_id_type=MESH)

    def inner_copy(k, first):
        a = first * half + (first * (half - 1) + k * (1 - 2 * first))
        q = 1 - first
        ref = sbuf.at[q, a, :, pl.ds(rows.faces, m * m)]
        return pltpu.make_async_remote_copy(
            src_ref=ref, dst_ref=ref, send_sem=isend.at[k],
            recv_sem=irecv.at[k], device_id=peer, device_id_type=MESH)

    def weigh(i, j, slot):
        flux[slot] = (geo[0, j, i] * vel[0, i] + geo[1, j, i] * vel[1, i]
                      + geo[2, j, i] * vel[2, i])

    def first_flux(k, carry):
        i = plane_at(k)
        a = h * half + i
        load(k, 0).wait()
        load(k, 1).wait()
        weigh(i, 0, 0)
        for q in range(2):
            for t in range(tiles):
                fbuf[q, a, t, pl.ds(0, rows.plane), :] = flux[0, pl.ds(t * 2 + q, rows.plane, stride=parts), :]
        flux_copy(k, h).start()
        return carry

    lax.fori_loop(0, half, first_flux, 0)

    stack[...] = jnp.zeros_like(stack)

    def plane_terms(k, carry):
        i = plane_at(k)
        a = h * half + i
        load(k, 2).wait()
        weigh(i, 1, 0)
        weigh(i, 2, 1)
        tall = up(rows.total, 8)
        for q in range(2):
            for j in range(2):
                for t in range(tiles):
                    stack[q, pl.ds(j * rows.plane_pad, rows.plane), pl.ds(t * LANES, LANES)] = (
                        flux[j, pl.ds(t * 2 + q, rows.plane, stride=parts), :])
            high, low = halves(stack[q])
            both = dot(kmat_ref[...], high)
            term = both[:tall] + both[tall:] + dot(kmat_ref[pl.ds(0, tall)], low)
            for t in range(tiles):
                sbuf[q, a, t] = term[:, t * LANES:(t + 1) * LANES]
        face_copy(k, h).start()

        @pl.when(k == 0)
        def _():
            inner_copy(0, h).start()
        return carry

    lax.fori_loop(0, half, plane_terms, 0)
    for k in range(1, half):
        inner_copy(k, h).start()

    lanes = tiles * LANES
    row = place_ref[...]
    col = jnp.transpose(
        jnp.broadcast_to(row.astype(jnp.float32), (LANES, lanes))).astype(jnp.int32)[:, :1]
    bx, by, bz = BLOCK

    def keys(p):
        x, y, z = p // (by * bz), (p // bz) % by, p % bz
        at, on = (x, y, z), (p % (by * bz), x * bz + z, p // bz)
        result = []
        for d in range(3):
            jump = (by * bz, bz, 1)[d]
            low, high = at[d] == 0, at[d] == BLOCK[d] - 1
            result.append((
                (jnp.where(low, AWAY, p - jump), jnp.where(low, on[d], AWAY)),
                (jnp.where(high, AWAY, p + jump), jnp.where(high, on[d], AWAY)),
            ))
        return result

    col_keys, row_keys = keys(col), keys(row)
    lane_at = lax.broadcasted_iota(jnp.int32, (lanes, LANES), 1)
    sub_at = lax.broadcasted_iota(jnp.int32, (LANES, lanes), 0)

    def onehot(verdict):
        return jnp.where(verdict, 1.0, 0.0).astype(jnp.bfloat16)

    for d in range(3):
        for side in range(2):
            near[d, side] = onehot(col_keys[d][side][0] == row)
            sel[d, side] = onehot(col_keys[d][side][1] == lane_at)
            selt[d, side] = onehot(sub_at == row_keys[d][side][1])

    def arrive_flux(k, carry):
        flux_copy(k, other).wait_recv()
        return carry

    lax.fori_loop(0, half, arrive_flux, 0)

    def along_first(g, carry):
        at = pl.ds(pl.multiple_of(g * 8, 8), 8)
        for t in range(tiles):
            values = [fbuf[h, i, t, at, :] for i in range(n)]
            for a in range(n):
                total = values[0] * float(table[0, a])
                for i in range(1, n):
                    total = total + values[i] * float(table[i, a])
                field[a, t, at, :] = total
        return carry

    lax.fori_loop(0, rows.plane_pad // 8, along_first, 0)

    def arrive_faces(k, carry):
        face_copy(k, other).wait_recv()
        return carry

    lax.fori_loop(0, half, arrive_faces, 0)
    inner_copy(0, other).wait_recv()

    def add_faces(a, carry):
        for t in range(tiles):
            for start, count, at in (
                (rows.c_low, m, pl.ds(n, m, stride=n)),
                (rows.c_high, m, pl.ds(2 * n - 1, m, stride=n)),
                (rows.b_low, n, pl.ds(0, n)),
                (rows.b_high, n, pl.ds(n * (n - 1), n)),
            ):
                field[a, t, at, :] = field[a, t, at, :] + sbuf[h, a, t, pl.ds(start, count), :]
        return carry

    lax.fori_loop(0, n, add_faces, 0)

    def add_inner(a):
        for t in range(tiles):
            for b in range(m):
                at = pl.ds(n * (b + 1) + 1, m)
                field[a, t, at, :] = (
                    field[a, t, at, :] + sbuf[h, a, t, pl.ds(rows.faces + b * m, m), :])

    add_inner(0)
    add_inner(n - 1)

    def take(d, side):
        node = side * (n - 1)
        if d == 0:
            return
        def one(a, carry):
            for t in range(tiles):
                at = pl.ds(node * n, n) if d == 1 else pl.ds(node, n, stride=n)
                face[side, t, pl.ds(a * n, n), :] = field[a, t, at, :]
            return carry
        lax.fori_loop(0, n, one, 0)

    def give(d, side, values):
        node = side * (n - 1)
        for t in range(tiles):
            piece = values[:, t * LANES:(t + 1) * LANES]
            if d == 0:
                field[node, t] = piece
            else:
                face[side, t] = piece
        if d == 0:
            return
        def one(a, carry):
            for t in range(tiles):
                at = pl.ds(node * n, n) if d == 1 else pl.ds(node, n, stride=n)
                field[a, t, at, :] = face[side, t, pl.ds(a * n, n), :]
            return carry
        lax.fori_loop(0, n, one, 0)

    def whole(d, side):
        source = field.at[side * (n - 1)] if d == 0 else face.at[side]
        return jnp.concatenate([source[t] for t in range(tiles)], axis=1)

    def step_copy(d, side):
        return pltpu.make_async_remote_copy(
            src_ref=outb.at[d, side], dst_ref=inb.at[d, 1 - side],
            send_sem=nsend.at[d, side], recv_sem=nrecv.at[d, 1 - side],
            device_id=neighbour(d, side), device_id_type=MESH)

    def step_arrival(d, side):
        return pltpu.make_async_remote_copy(
            src_ref=outb.at[d, side], dst_ref=inb.at[d, side],
            send_sem=nsend.at[d, side], recv_sem=nrecv.at[d, side],
            device_id=neighbour(d, side), device_id_type=MESH)

    for d in range(3):
        for side in range(2):
            take(d, side)
        split = []
        for side in range(2):
            values = whole(d, side)
            high, low = halves(values)
            split.append((values, high, low))
            outb[d, side] = dot(high, sel[d, side]) + dot(low, sel[d, side])

            @pl.when(has(d, side))
            def _():
                step_copy(d, side).start()
        totals = []
        for side in range(2):
            _, high, low = split[1 - side]
            totals.append(
                split[side][0] + (dot(high, near[d, 1 - side]) + dot(low, near[d, 1 - side])))
        for side in range(2):
            @pl.when(has(d, side))
            def _():
                step_arrival(d, side).wait_recv()

            @pl.when(jnp.logical_not(has(d, side)))
            def _():
                inb[d, side] = jnp.zeros(inb.shape[2:], jnp.float32)
        for side in range(2):
            give(d, side, totals[side] + pair_dot(inb[d, side], selt[d, side]))

    def arrive_inner(k, carry):
        inner_copy(k, other).wait_recv()
        return carry

    lax.fori_loop(1, half, arrive_inner, 0)

    def inner_planes(a, carry):
        add_inner(a)
        return carry

    lax.fori_loop(1, n - 1, inner_planes, 0)

    def put(a, carry):
        for t in range(tiles):
            out_ref[a, pl.ds(t, rows.plane, stride=tiles), :] = field[a, t, pl.ds(0, rows.plane), :]
        return carry

    lax.fori_loop(0, n, put, 0)

    for k in range(half):
        flux_copy(k, h).wait_send()
        face_copy(k, h).wait_send()
        inner_copy(k, h).wait_send()
    for d in range(3):
        for side in range(2):
            @pl.when(has(d, side))
            def _():
                step_copy(d, side).wait_send()


def body(velocity, geometry, element_place):
    comp_count, rep_count = lax.axis_size("comp"), lax.axis_size("rep")
    half, n = velocity.shape[1], velocity.shape[2]
    elems = velocity.shape[-1]
    tiles = elems // LANES
    table = np.asarray(derivative_table(n), np.float32)
    rows = Rows(n)
    parts = tiles * 2

    def view(x):
        lead = x.shape[:-4]
        x = x.reshape(lead + (n * n, 2, tiles, LANES))
        x = jnp.swapaxes(x, -2, -3)
        return x.reshape(lead + (n * n * parts, LANES))

    tall = up(rows.total, 8)
    deep = rows.plane_pad
    long = n * n * parts
    f32, bf16 = jnp.float32, jnp.bfloat16
    dma = pltpu.SemaphoreType.DMA
    result = pl.pallas_call(
        functools.partial(kernel, (n, half, tiles, table, rows, (comp_count, rep_count))),
        out_shape=jax.ShapeDtypeStruct((n, n * n * tiles, LANES), f32),
        in_specs=[
            pl.BlockSpec(memory_space=pltpu.VMEM),
            pl.BlockSpec(memory_space=pltpu.VMEM),
            pl.BlockSpec(memory_space=pl.ANY),
            pl.BlockSpec(memory_space=pl.ANY),
        ],
        out_specs=pl.BlockSpec(memory_space=pltpu.VMEM),
        scratch_shapes=[
            pltpu.VMEM((3, half, long, LANES), f32),
            pltpu.VMEM((3, 3, half, long, LANES), f32),
            pltpu.VMEM((2, long, LANES), f32),
            pltpu.VMEM((2, 2 * deep, elems), f32),
            pltpu.VMEM((2, n, tiles, deep, LANES), f32),
            pltpu.VMEM((2, n, tiles, tall, LANES), f32),
            pltpu.VMEM((n, tiles, deep, LANES), f32),
            pltpu.VMEM((2, tiles, deep, LANES), f32),
            pltpu.VMEM((3, 2, elems, elems), bf16),
            pltpu.VMEM((3, 2, elems, LANES), bf16),
            pltpu.VMEM((3, 2, LANES, elems), bf16),
            pltpu.VMEM((3, 2, deep, LANES), f32),
            pltpu.VMEM((3, 2, deep, LANES), f32),
            dma((3, half)),
            dma((half,)), dma((half,)), dma((half,)), dma((half,)), dma((half,)), dma((half,)),
            dma((3, 2)), dma((3, 2)),
        ],
        compiler_params=pltpu.CompilerParams(
            collective_id=0, has_side_effects=True, vmem_limit_bytes=60 * 1024 * 1024
        ),
    )(element_place, plane_matrix(table, rows), view(velocity), view(geometry))
    return result.reshape(n, n, n, 1, elems)


def solution(mesh):
    placed = (
        P(None, "comp", None, None, None, ("elem", "rep")),
        P(None, None, "comp", None, None, None, ("elem", "rep")),
        P("comp", ("elem", "rep")),
    )
    return jax.shard_map(
        body,
        mesh=mesh,
        in_specs=placed,
        out_specs=P(None, None, None, "comp", ("elem", "rep")),
        check_vma=False,
    )
```

```python
import functools

import jax
import jax.numpy as jnp
import numpy as np
from jax import lax
from jax.experimental import pallas as pl
from jax.experimental.layout import Layout, with_layout_constraint
from jax.experimental.pallas import tpu as pltpu
from jax.sharding import PartitionSpec as P

BLOCK = (6, 8, 8)
GRID_Y = 4
LANES = 128
MESH = pl.DeviceIdType.MESH
AWAY = -100000


def legendre_columns(points, degree):
    columns = [points * 0.0 + 1.0, points]
    for order in range(2, degree + 1):
        columns.append(
            ((2 * order - 1) * points * columns[order - 1] - (order - 1) * columns[order - 2])
            / order
        )
    return columns


def derivative_table(node_count):
    degree = node_count - 1
    points = np.cos(np.pi * np.arange(node_count) / degree)
    for sweep in range(100):
        columns = legendre_columns(points, degree)
        points = points - (points * columns[degree] - columns[degree - 1]) / (
            node_count * columns[degree]
        )
    points = np.sort(points)
    values = legendre_columns(points, degree)[degree]
    identity = np.eye(node_count)
    spacing = points[:, None] - points[None, :] + identity
    matrix = values[:, None] / (values[None, :] * spacing)
    matrix = np.where(identity > 0.5, 0.0, matrix)
    matrix[0, 0] = -degree * (degree + 1) / 4.0
    matrix[degree, degree] = degree * (degree + 1) / 4.0
    return matrix


def up(count, step):
    return -(-count // step) * step


class Rows:
    def __init__(self, n):
        self.n = n
        m = n - 2
        self.m = m
        self.c_low, self.c_high = 0, m
        self.b_low, self.b_high = 2 * m, 2 * m + n
        self.faces = up(2 * m + 2 * n, 8)
        self.plane = n * n
        self.plane_pad = up(n * n, 8)
        self.total = self.faces + m * m

    def nodes(self):
        n, m = self.n, self.m
        order = [None] * up(self.total, 8)
        for k in range(m):
            order[self.c_low + k] = (k + 1, 0)
            order[self.c_high + k] = (k + 1, n - 1)
        for k in range(n):
            order[self.b_low + k] = (0, k)
            order[self.b_high + k] = (n - 1, k)
        for b in range(m):
            for c in range(m):
                order[self.faces + b * m + c] = (b + 1, c + 1)
        return order


def plane_matrix(table, rows):
    n = rows.n
    order = rows.nodes()
    matrix = np.zeros((len(order), 2 * rows.plane_pad), np.float32)
    for r, node in enumerate(order):
        if node is not None:
            b, c = node
            for i in range(n):
                matrix[r, i * n + c] += table[i, b]
                matrix[r, rows.plane_pad + b * n + i] += table[i, c]
    top = jnp.asarray(matrix).astype(jnp.bfloat16)
    rest = (jnp.asarray(matrix) - top.astype(jnp.float32)).astype(jnp.bfloat16)
    return jnp.concatenate([top, rest], axis=0)


def halves(x):
    high = x.astype(jnp.bfloat16)
    low = (x - high.astype(jnp.float32)).astype(jnp.bfloat16)
    return high, low


def dot(a, b):
    return jnp.dot(a, b, preferred_element_type=jnp.float32)


def pair_dot(x, onehot):
    high, low = halves(x)
    return dot(high, onehot) + dot(low, onehot)


def kernel(sizes, place_ref, kmat_ref, vel_ref, geo_ref, out_ref,
           vel, geo, flux, stack, fbuf, sbuf, field, face, near, sel, selt, outb, inb,
           load_sem, fsend, frecv, ssend, srecv, isend, irecv, nsend, nrecv):
    n, half, tiles, table, rows, counts = sizes
    m = rows.m
    parts = tiles * 2
    comp_count, rep_count = counts
    e, h, r = lax.axis_index("elem"), lax.axis_index("comp"), lax.axis_index("rep")
    elem_count = lax.axis_size("elem")
    other = 1 - h
    layers = comp_count * rep_count
    device = e * layers + h * rep_count + r
    stride_x = GRID_Y * layers
    extents = (elem_count * layers // stride_x, GRID_Y, layers)
    strides = (stride_x, layers, 1)
    position = (device // stride_x, (device // layers) % GRID_Y, device % layers)

    def coords(target):
        return (target // layers, (target // rep_count) % comp_count, target % rep_count)

    def has(d, side):
        if side == 0:
            return position[d] > 0
        return position[d] < extents[d] - 1

    def neighbour(d, side):
        return coords(device + (strides[d] if side == 1 else -strides[d]))

    def plane_at(k):
        return h * (half - 1) + k * (1 - 2 * h)

    def load(k, what):
        i = plane_at(k)
        if what == 0:
            return pltpu.make_async_copy(vel_ref.at[:, i], vel.at[:, i], load_sem.at[0, k])
        if what == 1:
            return pltpu.make_async_copy(geo_ref.at[:, 0, i], geo.at[:, 0, i], load_sem.at[1, k])
        return pltpu.make_async_copy(
            geo_ref.at[:, pl.ds(1, 2), i], geo.at[:, pl.ds(1, 2), i], load_sem.at[2, k]
        )

    for k in range(half):
        load(k, 0).start()
        load(k, 1).start()
    for k in range(half):
        load(k, 2).start()

    barrier = pltpu.get_barrier_semaphore()
    pl.semaphore_signal(barrier, inc=1, device_id=(e, other, r), device_id_type=MESH)
    expected = jnp.int32(1)
    for d in range(3):
        for side in range(2):
            @pl.when(has(d, side))
            def _():
                pl.semaphore_signal(
                    barrier, inc=1, device_id=neighbour(d, side), device_id_type=MESH
                )
            expected = expected + has(d, side).astype(jnp.int32)
    pl.semaphore_wait(barrier, expected)

    peer = (e, other, r)

    def flux_copy(k, first):
        a = first * half + (first * (half - 1) + k * (1 - 2 * first))
        q = 1 - first
        return pltpu.make_async_remote_copy(
            src_ref=fbuf.at[q, a], dst_ref=fbuf.at[q, a], send_sem=fsend.at[k],
            recv_sem=frecv.at[k], device_id=peer, device_id_type=MESH)

    def face_copy(k, first):
        a = first * half + (first * (half - 1) + k * (1 - 2 * first))
        q = 1 - first
        ref = sbuf.at[q, a, :, pl.ds(0, rows.faces)]
        return pltpu.make_async_remote_copy(
            src_ref=ref, dst_ref=ref, send_sem=ssend.at[k],
            recv_sem=srecv.at[k], device_id=peer, device_id_type=MESH)

    def inner_copy(k, first):
        a = first * half + (first * (half - 1) + k * (1 - 2 * first))
        q = 1 - first
        ref = sbuf.at[q, a, :, pl.ds(rows.faces, m * m)]
        return pltpu.make_async_remote_copy(
            src_ref=ref, dst_ref=ref, send_sem=isend.at[k],
            recv_sem=irecv.at[k], device_id=peer, device_id_type=MESH)

    def weigh(i, j, slot):
        flux[slot] = (geo[0, j, i] * vel[0, i] + geo[1, j, i] * vel[1, i]
                      + geo[2, j, i] * vel[2, i])

    def first_flux(k, carry):
        i = plane_at(k)
        a = h * half + i
        load(k, 0).wait()
        load(k, 1).wait()
        weigh(i, 0, 0)
        for q in range(2):
            for t in range(tiles):
                fbuf[q, a, t, pl.ds(0, rows.plane), :] = flux[0, pl.ds(t * 2 + q, rows.plane, stride=parts), :]
        flux_copy(k, h).start()
        return carry

    lax.fori_loop(0, half, first_flux, 0)

    stack[...] = jnp.zeros_like(stack)

    def plane_terms(k, carry):
        i = plane_at(k)
        a = h * half + i
        load(k, 2).wait()
        weigh(i, 1, 0)
        weigh(i, 2, 1)
        tall = up(rows.total, 8)
        for q in range(2):
            for j in range(2):
                for t in range(tiles):
                    stack[q, pl.ds(j * rows.plane_pad, rows.plane), pl.ds(t * LANES, LANES)] = (
                        flux[j, pl.ds(t * 2 + q, rows.plane, stride=parts), :])
            high, low = halves(stack[q])
            both = dot(kmat_ref[...], high)
            term = both[:tall] + both[tall:] + dot(kmat_ref[pl.ds(0, tall)], low)
            for t in range(tiles):
                sbuf[q, a, t] = term[:, t * LANES:(t + 1) * LANES]
        face_copy(k, h).start()

        @pl.when(k == 0)
        def _():
            inner_copy(0, h).start()
        return carry

    lax.fori_loop(0, half, plane_terms, 0)
    for k in range(1, half):
        inner_copy(k, h).start()

    lanes = tiles * LANES
    row = place_ref[...]
    col = jnp.transpose(
        jnp.broadcast_to(row.astype(jnp.float32), (LANES, lanes))).astype(jnp.int32)[:, :1]
    bx, by, bz = BLOCK

    def keys(p):
        x, y, z = p // (by * bz), (p // bz) % by, p % bz
        at, on = (x, y, z), (p % (by * bz), x * bz + z, p // bz)
        result = []
        for d in range(3):
            jump = (by * bz, bz, 1)[d]
            low, high = at[d] == 0, at[d] == BLOCK[d] - 1
            result.append((
                (jnp.where(low, AWAY, p - jump), jnp.where(low, on[d], AWAY)),
                (jnp.where(high, AWAY, p + jump), jnp.where(high, on[d], AWAY)),
            ))
        return result

    col_keys, row_keys = keys(col), keys(row)
    lane_at = lax.broadcasted_iota(jnp.int32, (lanes, LANES), 1)
    sub_at = lax.broadcasted_iota(jnp.int32, (LANES, lanes), 0)

    def onehot(verdict):
        return jnp.where(verdict, 1.0, 0.0).astype(jnp.bfloat16)

    for d in range(3):
        for side in range(2):
            near[d, side] = onehot(col_keys[d][side][0] == row)
            sel[d, side] = onehot(col_keys[d][side][1] == lane_at)
            selt[d, side] = onehot(sub_at == row_keys[d][side][1])

    def arrive_flux(k, carry):
        flux_copy(k, other).wait_recv()
        return carry

    lax.fori_loop(0, half, arrive_flux, 0)

    def along_first(g, carry):
        at = pl.ds(pl.multiple_of(g * 8, 8), 8)
        for t in range(tiles):
            values = [fbuf[h, i, t, at, :] for i in range(n)]
            for a in range(n):
                total = values[0] * float(table[0, a])
                for i in range(1, n):
                    total = total + values[i] * float(table[i, a])
                field[a, t, at, :] = total
        return carry

    lax.fori_loop(0, rows.plane_pad // 8, along_first, 0)

    def arrive_faces(k, carry):
        face_copy(k, other).wait_recv()
        return carry

    lax.fori_loop(0, half, arrive_faces, 0)
    inner_copy(0, other).wait_recv()

    def add_faces(a, carry):
        for t in range(tiles):
            for start, count, at in (
                (rows.c_low, m, pl.ds(n, m, stride=n)),
                (rows.c_high, m, pl.ds(2 * n - 1, m, stride=n)),
                (rows.b_low, n, pl.ds(0, n)),
                (rows.b_high, n, pl.ds(n * (n - 1), n)),
            ):
                field[a, t, at, :] = field[a, t, at, :] + sbuf[h, a, t, pl.ds(start, count), :]
        return carry

    lax.fori_loop(0, n, add_faces, 0)

    def add_inner(a):
        for t in range(tiles):
            for b in range(m):
                at = pl.ds(n * (b + 1) + 1, m)
                field[a, t, at, :] = (
                    field[a, t, at, :] + sbuf[h, a, t, pl.ds(rows.faces + b * m, m), :])

    add_inner(0)
    add_inner(n - 1)

    def take(d, side):
        node = side * (n - 1)
        if d == 0:
            return
        def one(a, carry):
            for t in range(tiles):
                at = pl.ds(node * n, n) if d == 1 else pl.ds(node, n, stride=n)
                face[side, t, pl.ds(a * n, n), :] = field[a, t, at, :]
            return carry
        lax.fori_loop(0, n, one, 0)

    def give(d, side, values):
        node = side * (n - 1)
        for t in range(tiles):
            piece = values[:, t * LANES:(t + 1) * LANES]
            if d == 0:
                field[node, t] = piece
            else:
                face[side, t] = piece
        if d == 0:
            return
        def one(a, carry):
            for t in range(tiles):
                at = pl.ds(node * n, n) if d == 1 else pl.ds(node, n, stride=n)
                field[a, t, at, :] = face[side, t, pl.ds(a * n, n), :]
            return carry
        lax.fori_loop(0, n, one, 0)

    def whole(d, side):
        source = field.at[side * (n - 1)] if d == 0 else face.at[side]
        return jnp.concatenate([source[t] for t in range(tiles)], axis=1)

    def step_copy(d, side):
        return pltpu.make_async_remote_copy(
            src_ref=outb.at[d, side], dst_ref=inb.at[d, 1 - side],
            send_sem=nsend.at[d, side], recv_sem=nrecv.at[d, 1 - side],
            device_id=neighbour(d, side), device_id_type=MESH)

    def step_arrival(d, side):
        return pltpu.make_async_remote_copy(
            src_ref=outb.at[d, side], dst_ref=inb.at[d, side],
            send_sem=nsend.at[d, side], recv_sem=nrecv.at[d, side],
            device_id=neighbour(d, side), device_id_type=MESH)

    for d in range(3):
        for side in range(2):
            take(d, side)
        split = []
        for side in range(2):
            values = whole(d, side)
            high, low = halves(values)
            split.append((values, high, low))
            outb[d, side] = dot(high, sel[d, side]) + dot(low, sel[d, side])

            @pl.when(has(d, side))
            def _():
                step_copy(d, side).start()
        totals = []
        for side in range(2):
            _, high, low = split[1 - side]
            totals.append(
                split[side][0] + (dot(high, near[d, 1 - side]) + dot(low, near[d, 1 - side])))
        for side in range(2):
            @pl.when(has(d, side))
            def _():
                step_arrival(d, side).wait_recv()

            @pl.when(jnp.logical_not(has(d, side)))
            def _():
                inb[d, side] = jnp.zeros(inb.shape[2:], jnp.float32)
        for side in range(2):
            give(d, side, totals[side] + pair_dot(inb[d, side], selt[d, side]))

    def arrive_inner(k, carry):
        inner_copy(k, other).wait_recv()
        return carry

    lax.fori_loop(1, half, arrive_inner, 0)

    def inner_planes(a, carry):
        add_inner(a)
        return carry

    lax.fori_loop(1, n - 1, inner_planes, 0)

    def put(a, carry):
        for t in range(tiles):
            out_ref[a, pl.ds(t, rows.plane, stride=tiles), :] = field[a, t, pl.ds(0, rows.plane), :]
        return carry

    lax.fori_loop(0, n, put, 0)

    for k in range(half):
        flux_copy(k, h).wait_send()
        face_copy(k, h).wait_send()
        inner_copy(k, h).wait_send()
    for d in range(3):
        for side in range(2):
            @pl.when(has(d, side))
            def _():
                step_copy(d, side).wait_send()


def body(velocity, geometry, element_place):
    comp_count, rep_count = lax.axis_size("comp"), lax.axis_size("rep")
    half, n = velocity.shape[1], velocity.shape[2]
    elems = velocity.shape[-1]
    tiles = elems // LANES
    table = np.asarray(derivative_table(n), np.float32)
    rows = Rows(n)
    parts = tiles * 2

    def view(x):
        lead = x.shape[:-4]
        x = x.reshape(lead + (n * n, 2, tiles, LANES))
        rank = len(lead)
        order = tuple(range(rank + 1)) + (rank + 2, rank + 1, rank + 3)
        x = with_layout_constraint(x, Layout(major_to_minor=order))
        x = jnp.swapaxes(x, -2, -3)
        return x.reshape(lead + (n * n * parts, LANES))

    tall = up(rows.total, 8)
    deep = rows.plane_pad
    long = n * n * parts
    f32, bf16 = jnp.float32, jnp.bfloat16
    dma = pltpu.SemaphoreType.DMA
    result = pl.pallas_call(
        functools.partial(kernel, (n, half, tiles, table, rows, (comp_count, rep_count))),
        out_shape=jax.ShapeDtypeStruct((n, n * n * tiles, LANES), f32),
        in_specs=[
            pl.BlockSpec(memory_space=pltpu.VMEM),
            pl.BlockSpec(memory_space=pltpu.VMEM),
            pl.BlockSpec(memory_space=pl.ANY),
            pl.BlockSpec(memory_space=pl.ANY),
        ],
        out_specs=pl.BlockSpec(memory_space=pltpu.VMEM),
        scratch_shapes=[
            pltpu.VMEM((3, half, long, LANES), f32),
            pltpu.VMEM((3, 3, half, long, LANES), f32),
            pltpu.VMEM((2, long, LANES), f32),
            pltpu.VMEM((2, 2 * deep, elems), f32),
            pltpu.VMEM((2, n, tiles, deep, LANES), f32),
            pltpu.VMEM((2, n, tiles, tall, LANES), f32),
            pltpu.VMEM((n, tiles, deep, LANES), f32),
            pltpu.VMEM((2, tiles, deep, LANES), f32),
            pltpu.VMEM((3, 2, elems, elems), bf16),
            pltpu.VMEM((3, 2, elems, LANES), bf16),
            pltpu.VMEM((3, 2, LANES, elems), bf16),
            pltpu.VMEM((3, 2, deep, LANES), f32),
            pltpu.VMEM((3, 2, deep, LANES), f32),
            dma((3, half)),
            dma((half,)), dma((half,)), dma((half,)), dma((half,)), dma((half,)), dma((half,)),
            dma((3, 2)), dma((3, 2)),
        ],
        compiler_params=pltpu.CompilerParams(
            collective_id=0, has_side_effects=True, vmem_limit_bytes=60 * 1024 * 1024
        ),
    )(element_place, plane_matrix(table, rows), view(velocity), view(geometry))
    return result.reshape(n, n, n, 1, elems)


def solution(mesh):
    placed = (
        P(None, "comp", None, None, None, ("elem", "rep")),
        P(None, None, "comp", None, None, None, ("elem", "rep")),
        P("comp", ("elem", "rep")),
    )
    return jax.shard_map(
        body,
        mesh=mesh,
        in_specs=placed,
        out_specs=P(None, None, None, "comp", ("elem", "rep")),
        check_vma=False,
    )
```

```python
import functools

import jax
import jax.numpy as jnp
import numpy as np
from jax import lax
from jax.experimental import pallas as pl
from jax.experimental.layout import Layout, with_layout_constraint
from jax.experimental.pallas import tpu as pltpu
from jax.sharding import PartitionSpec as P

BLOCK = (6, 8, 8)
GRID_Y = 4
LANES = 128
MESH = pl.DeviceIdType.MESH
AWAY = -100000


def legendre_columns(points, degree):
    columns = [points * 0.0 + 1.0, points]
    for order in range(2, degree + 1):
        columns.append(
            ((2 * order - 1) * points * columns[order - 1] - (order - 1) * columns[order - 2])
            / order
        )
    return columns


def derivative_table(node_count):
    degree = node_count - 1
    points = np.cos(np.pi * np.arange(node_count) / degree)
    for sweep in range(100):
        columns = legendre_columns(points, degree)
        points = points - (points * columns[degree] - columns[degree - 1]) / (
            node_count * columns[degree]
        )
    points = np.sort(points)
    values = legendre_columns(points, degree)[degree]
    identity = np.eye(node_count)
    spacing = points[:, None] - points[None, :] + identity
    matrix = values[:, None] / (values[None, :] * spacing)
    matrix = np.where(identity > 0.5, 0.0, matrix)
    matrix[0, 0] = -degree * (degree + 1) / 4.0
    matrix[degree, degree] = degree * (degree + 1) / 4.0
    return matrix


def up(count, step):
    return -(-count // step) * step


class Rows:
    def __init__(self, n):
        self.n = n
        m = n - 2
        self.m = m
        self.c_low, self.c_high = 0, m
        self.b_low, self.b_high = 2 * m, 2 * m + n
        self.faces = up(2 * m + 2 * n, 8)
        self.plane = n * n
        self.plane_pad = up(n * n, 8)
        self.total = self.faces + m * m

    def nodes(self):
        n, m = self.n, self.m
        order = [None] * up(self.total, 8)
        for k in range(m):
            order[self.c_low + k] = (k + 1, 0)
            order[self.c_high + k] = (k + 1, n - 1)
        for k in range(n):
            order[self.b_low + k] = (0, k)
            order[self.b_high + k] = (n - 1, k)
        for b in range(m):
            for c in range(m):
                order[self.faces + b * m + c] = (b + 1, c + 1)
        return order


def plane_matrix(table, rows):
    n = rows.n
    order = rows.nodes()
    matrix = np.zeros((len(order), 2 * rows.plane_pad), np.float32)
    for r, node in enumerate(order):
        if node is not None:
            b, c = node
            for i in range(n):
                matrix[r, i * n + c] += table[i, b]
                matrix[r, rows.plane_pad + b * n + i] += table[i, c]
    top = jnp.asarray(matrix).astype(jnp.bfloat16)
    rest = (jnp.asarray(matrix) - top.astype(jnp.float32)).astype(jnp.bfloat16)
    return jnp.concatenate([top, rest], axis=0)


def halves(x):
    high = x.astype(jnp.bfloat16)
    low = (x - high.astype(jnp.float32)).astype(jnp.bfloat16)
    return high, low


def dot(a, b):
    return jnp.dot(a, b, preferred_element_type=jnp.float32)


def pair_dot(x, onehot):
    high, low = halves(x)
    return dot(high, onehot) + dot(low, onehot)


def kernel(sizes, place_ref, kmat_ref, vel_ref, geo_ref, out_ref,
           vel, geo, flux, stack, fbuf, sbuf, field, face, near, sel, selt, outb, inb,
           ready, load_sem, fsend, frecv, ssend, srecv, isend, irecv, nsend, nrecv, out_sem):
    n, half, tiles, table, rows, counts = sizes
    m = rows.m
    parts = tiles * 2
    comp_count, rep_count = counts
    e, h, r = lax.axis_index("elem"), lax.axis_index("comp"), lax.axis_index("rep")
    elem_count = lax.axis_size("elem")
    other = 1 - h
    layers = comp_count * rep_count
    device = e * layers + h * rep_count + r
    stride_x = GRID_Y * layers
    extents = (elem_count * layers // stride_x, GRID_Y, layers)
    strides = (stride_x, layers, 1)
    position = (device // stride_x, (device // layers) % GRID_Y, device % layers)

    def coords(target):
        return (target // layers, (target // rep_count) % comp_count, target % rep_count)

    def has(d, side):
        if side == 0:
            return position[d] > 0
        return position[d] < extents[d] - 1

    def neighbour(d, side):
        return coords(device + (strides[d] if side == 1 else -strides[d]))

    def plane_at(k):
        return h * (half - 1) + k * (1 - 2 * h)

    def load(k, what):
        i = plane_at(k)
        if what == 0:
            return pltpu.make_async_copy(vel_ref.at[:, i], vel.at[:, i], load_sem.at[0, k])
        if what == 1:
            return pltpu.make_async_copy(geo_ref.at[:, 0, i], geo.at[:, 0, i], load_sem.at[1, k])
        return pltpu.make_async_copy(
            geo_ref.at[:, pl.ds(1, 2), i], geo.at[:, pl.ds(1, 2), i], load_sem.at[2, k]
        )

    for k in range(half):
        load(k, 0).start()
        load(k, 1).start()
    for k in range(half):
        load(k, 2).start()

    barrier = pltpu.get_barrier_semaphore()
    pl.semaphore_signal(barrier, inc=1, device_id=(e, other, r), device_id_type=MESH)
    expected = jnp.int32(1)
    for d in range(3):
        for side in range(2):
            @pl.when(has(d, side))
            def _():
                pl.semaphore_signal(
                    barrier, inc=1, device_id=neighbour(d, side), device_id_type=MESH
                )
            expected = expected + has(d, side).astype(jnp.int32)
    pl.semaphore_wait(barrier, expected)

    peer = (e, other, r)

    def flux_copy(k, first):
        a = first * half + (first * (half - 1) + k * (1 - 2 * first))
        q = 1 - first
        return pltpu.make_async_remote_copy(
            src_ref=fbuf.at[q, a], dst_ref=fbuf.at[q, a], send_sem=fsend.at[k],
            recv_sem=frecv.at[k], device_id=peer, device_id_type=MESH)

    def face_copy(k, first):
        a = first * half + (first * (half - 1) + k * (1 - 2 * first))
        q = 1 - first
        ref = sbuf.at[q, a, :, pl.ds(0, rows.faces)]
        return pltpu.make_async_remote_copy(
            src_ref=ref, dst_ref=ref, send_sem=ssend.at[k],
            recv_sem=srecv.at[k], device_id=peer, device_id_type=MESH)

    def inner_copy(k, first):
        a = first * half + (first * (half - 1) + k * (1 - 2 * first))
        q = 1 - first
        ref = sbuf.at[q, a, :, pl.ds(rows.faces, m * m)]
        return pltpu.make_async_remote_copy(
            src_ref=ref, dst_ref=ref, send_sem=isend.at[k],
            recv_sem=irecv.at[k], device_id=peer, device_id_type=MESH)

    def weigh(i, j, slot):
        flux[slot] = (geo[0, j, i] * vel[0, i] + geo[1, j, i] * vel[1, i]
                      + geo[2, j, i] * vel[2, i])

    def first_flux(k, carry):
        i = plane_at(k)
        a = h * half + i
        load(k, 0).wait()
        load(k, 1).wait()
        weigh(i, 0, 0)
        for q in range(2):
            for t in range(tiles):
                fbuf[q, a, t, pl.ds(0, rows.plane), :] = flux[0, pl.ds(t * 2 + q, rows.plane, stride=parts), :]
        flux_copy(k, h).start()
        return carry

    lax.fori_loop(0, half, first_flux, 0)

    stack[...] = jnp.zeros_like(stack)

    def plane_terms(k, carry):
        i = plane_at(k)
        a = h * half + i
        load(k, 2).wait()
        weigh(i, 1, 0)
        weigh(i, 2, 1)
        tall = up(rows.total, 8)
        for q in range(2):
            for j in range(2):
                for t in range(tiles):
                    stack[q, pl.ds(j * rows.plane_pad, rows.plane), pl.ds(t * LANES, LANES)] = (
                        flux[j, pl.ds(t * 2 + q, rows.plane, stride=parts), :])
            high, low = halves(stack[q])
            both = dot(kmat_ref[...], high)
            term = both[:tall] + both[tall:] + dot(kmat_ref[pl.ds(0, tall)], low)
            for t in range(tiles):
                sbuf[q, a, t] = term[:, t * LANES:(t + 1) * LANES]
        face_copy(k, h).start()

        @pl.when(k == 0)
        def _():
            inner_copy(0, h).start()
        return carry

    lax.fori_loop(0, half, plane_terms, 0)
    for k in range(1, half - 1):
        inner_copy(k, h).start()

    lanes = tiles * LANES
    row = place_ref[...]
    col = jnp.transpose(
        jnp.broadcast_to(row.astype(jnp.float32), (LANES, lanes))).astype(jnp.int32)[:, :1]
    bx, by, bz = BLOCK

    def keys(p):
        x, y, z = p // (by * bz), (p // bz) % by, p % bz
        at, on = (x, y, z), (p % (by * bz), x * bz + z, p // bz)
        result = []
        for d in range(3):
            jump = (by * bz, bz, 1)[d]
            low, high = at[d] == 0, at[d] == BLOCK[d] - 1
            result.append((
                (jnp.where(low, AWAY, p - jump), jnp.where(low, on[d], AWAY)),
                (jnp.where(high, AWAY, p + jump), jnp.where(high, on[d], AWAY)),
            ))
        return result

    col_keys, row_keys = keys(col), keys(row)
    lane_at = lax.broadcasted_iota(jnp.int32, (lanes, LANES), 1)
    sub_at = lax.broadcasted_iota(jnp.int32, (LANES, lanes), 0)

    def onehot(verdict):
        return jnp.where(verdict, 1.0, 0.0).astype(jnp.bfloat16)

    for d in range(3):
        for side in range(2):
            near[d, side] = onehot(col_keys[d][side][0] == row)
            sel[d, side] = onehot(col_keys[d][side][1] == lane_at)
            selt[d, side] = onehot(sub_at == row_keys[d][side][1])

    def arrive_flux(k, carry):
        flux_copy(k, other).wait_recv()
        return carry

    lax.fori_loop(0, half, arrive_flux, 0)

    def along_first(g, carry):
        at = pl.ds(pl.multiple_of(g * 8, 8), 8)
        for t in range(tiles):
            values = [fbuf[h, i, t, at, :] for i in range(n)]
            for a in range(n):
                total = values[0] * float(table[0, a])
                for i in range(1, n):
                    total = total + values[i] * float(table[i, a])
                field[a, t, at, :] = total
        return carry

    lax.fori_loop(0, rows.plane_pad // 8, along_first, 0)

    def add_faces(a, carry):
        for t in range(tiles):
            for start, count, at in (
                (rows.c_low, m, pl.ds(n, m, stride=n)),
                (rows.c_high, m, pl.ds(2 * n - 1, m, stride=n)),
                (rows.b_low, n, pl.ds(0, n)),
                (rows.b_high, n, pl.ds(n * (n - 1), n)),
            ):
                field[a, t, at, :] = field[a, t, at, :] + sbuf[h, a, t, pl.ds(start, count), :]
        return carry

    def add_inner(a):
        for t in range(tiles):
            for b in range(m):
                at = pl.ds(n * (b + 1) + 1, m)
                field[a, t, at, :] = (
                    field[a, t, at, :] + sbuf[h, a, t, pl.ds(rows.faces + b * m, m), :])

    face_copy(0, other).wait_recv()
    inner_copy(0, other).wait_recv()
    for a in (0, n - 1):
        add_faces(a, 0)
        add_inner(a)

    def take(d, side):
        node = side * (n - 1)
        if d == 0:
            return
        def one(a, carry):
            for t in range(tiles):
                at = pl.ds(node * n, n) if d == 1 else pl.ds(node, n, stride=n)
                face[side, t, pl.ds(a * n, n), :] = field[a, t, at, :]
            return carry
        lax.fori_loop(0, n, one, 0)

    def give(d, side, values):
        node = side * (n - 1)
        for t in range(tiles):
            piece = values[:, t * LANES:(t + 1) * LANES]
            if d == 0:
                field[node, t] = piece
            else:
                face[side, t] = piece
        if d == 0:
            return
        def one(a, carry):
            for t in range(tiles):
                at = pl.ds(node * n, n) if d == 1 else pl.ds(node, n, stride=n)
                field[a, t, at, :] = face[side, t, pl.ds(a * n, n), :]
            return carry
        lax.fori_loop(0, n, one, 0)

    def whole(d, side):
        source = field.at[side * (n - 1)] if d == 0 else face.at[side]
        return jnp.concatenate([source[t] for t in range(tiles)], axis=1)

    def step_copy(d, side):
        return pltpu.make_async_remote_copy(
            src_ref=outb.at[d, side], dst_ref=inb.at[d, 1 - side],
            send_sem=nsend.at[d, side], recv_sem=nrecv.at[d, 1 - side],
            device_id=neighbour(d, side), device_id_type=MESH)

    def step_arrival(d, side):
        return pltpu.make_async_remote_copy(
            src_ref=outb.at[d, side], dst_ref=inb.at[d, side],
            send_sem=nsend.at[d, side], recv_sem=nrecv.at[d, side],
            device_id=neighbour(d, side), device_id_type=MESH)

    def arrive_faces(k, carry):
        face_copy(k, other).wait_recv()
        add_faces(other * half + other * (half - 1) + k * (1 - 2 * other), 0)
        return carry

    def own_faces(k, carry):
        add_faces(h * half + plane_at(k), 0)
        return carry

    def own_inner(k, carry):
        add_inner(h * half + plane_at(k))
        return carry

    for d in range(3):
        if d == 1:
            lax.fori_loop(1, half, arrive_faces, 0)
        for side in range(2):
            take(d, side)
        split = []
        for side in range(2):
            values = whole(d, side)
            high, low = halves(values)
            split.append((values, high, low))
            outb[d, side] = dot(high, sel[d, side]) + dot(low, sel[d, side])

            @pl.when(has(d, side))
            def _():
                step_copy(d, side).start()
        if d == 2:
            inner_copy(half - 1, h).start()
        totals = []
        for side in range(2):
            _, high, low = split[1 - side]
            totals.append(
                split[side][0] + (dot(high, near[d, 1 - side]) + dot(low, near[d, 1 - side])))
        if d == 0:
            lax.fori_loop(1, half, own_faces, 0)
        if d == 1:
            lax.fori_loop(1, half, own_inner, 0)
        for side in range(2):
            @pl.when(has(d, side))
            def _():
                step_arrival(d, side).wait_recv()

            @pl.when(jnp.logical_not(has(d, side)))
            def _():
                inb[d, side] = jnp.zeros(inb.shape[2:], jnp.float32)
        for side in range(2):
            give(d, side, totals[side] + pair_dot(inb[d, side], selt[d, side]))

    def put_copy(p):
        return pltpu.make_async_copy(ready.at[p], out_ref.at[p], out_sem.at[p])

    def put(a):
        first = (a % 2) * (rows.plane * tiles)
        for t in range(tiles):
            ready[a // 2, pl.ds(first + t, rows.plane, stride=tiles), :] = (
                field[a, t, pl.ds(0, rows.plane), :])

    put(0)
    put(n - 1)

    def put_own(k, carry):
        put(h * half + plane_at(k))
        return carry

    lax.fori_loop(1, half, put_own, 0)
    for p in range(half // 2):
        put_copy(h * (n // 2 - half // 2) + p).start()
    for k in range(1, half):
        a = other * half + other * (half - 1) + k * (1 - 2 * other)
        inner_copy(k, other).wait_recv()
        add_inner(a)
        put(a)
        if k % 2 == 1:
            put_copy(a // 2).start()
    if half % 2 == 1:
        put_copy(half // 2).start()
    for p in range(n // 2):
        put_copy(p).wait()

    for k in range(half):
        flux_copy(k, h).wait_send()
        face_copy(k, h).wait_send()
        inner_copy(k, h).wait_send()
    for d in range(3):
        for side in range(2):
            @pl.when(has(d, side))
            def _():
                step_copy(d, side).wait_send()


def body(velocity, geometry, element_place):
    comp_count, rep_count = lax.axis_size("comp"), lax.axis_size("rep")
    half, n = velocity.shape[1], velocity.shape[2]
    elems = velocity.shape[-1]
    tiles = elems // LANES
    table = np.asarray(derivative_table(n), np.float32)
    rows = Rows(n)
    parts = tiles * 2

    def view(x):
        lead = x.shape[:-4]
        x = x.reshape(lead + (n * n, 2, tiles, LANES))
        rank = len(lead)
        order = tuple(range(rank + 1)) + (rank + 2, rank + 1, rank + 3)
        x = with_layout_constraint(x, Layout(major_to_minor=order))
        x = jnp.swapaxes(x, -2, -3)
        return x.reshape(lead + (n * n * parts, LANES))

    tall = up(rows.total, 8)
    deep = rows.plane_pad
    long = n * n * parts
    f32, bf16 = jnp.float32, jnp.bfloat16
    dma = pltpu.SemaphoreType.DMA
    result = pl.pallas_call(
        functools.partial(kernel, (n, half, tiles, table, rows, (comp_count, rep_count))),
        out_shape=jax.ShapeDtypeStruct((n // 2, 2 * n * n * tiles, LANES), f32),
        in_specs=[
            pl.BlockSpec(memory_space=pltpu.VMEM),
            pl.BlockSpec(memory_space=pltpu.VMEM),
            pl.BlockSpec(memory_space=pl.ANY),
            pl.BlockSpec(memory_space=pl.ANY),
        ],
        out_specs=pl.BlockSpec(memory_space=pl.ANY),
        scratch_shapes=[
            pltpu.VMEM((3, half, long, LANES), f32),
            pltpu.VMEM((3, 3, half, long, LANES), f32),
            pltpu.VMEM((2, long, LANES), f32),
            pltpu.VMEM((2, 2 * deep, elems), f32),
            pltpu.VMEM((2, n, tiles, deep, LANES), f32),
            pltpu.VMEM((2, n, tiles, tall, LANES), f32),
            pltpu.VMEM((n, tiles, deep, LANES), f32),
            pltpu.VMEM((2, tiles, deep, LANES), f32),
            pltpu.VMEM((3, 2, elems, elems), bf16),
            pltpu.VMEM((3, 2, elems, LANES), bf16),
            pltpu.VMEM((3, 2, LANES, elems), bf16),
            pltpu.VMEM((3, 2, deep, LANES), f32),
            pltpu.VMEM((3, 2, deep, LANES), f32),
            pltpu.VMEM((n // 2, 2 * n * n * tiles, LANES), f32),
            dma((3, half)),
            dma((half,)), dma((half,)), dma((half,)), dma((half,)), dma((half,)), dma((half,)),
            dma((3, 2)), dma((3, 2)), dma((n // 2,)),
        ],
        compiler_params=pltpu.CompilerParams(
            collective_id=0, has_side_effects=True, vmem_limit_bytes=60 * 1024 * 1024
        ),
    )(element_place, plane_matrix(table, rows), view(velocity), view(geometry))
    result = jnp.swapaxes(result.reshape(n, n, n, tiles, 1, LANES), 3, 4)
    result = with_layout_constraint(result, Layout(major_to_minor=(0, 1, 2, 4, 3, 5)))
    return result.reshape(n, n, n, 1, elems)


def solution(mesh):
    placed = (
        P(None, "comp", None, None, None, ("elem", "rep")),
        P(None, None, "comp", None, None, None, ("elem", "rep")),
        P("comp", ("elem", "rep")),
    )
    return jax.shard_map(
        body,
        mesh=mesh,
        in_specs=placed,
        out_specs=P(None, None, None, "comp", ("elem", "rep")),
        check_vma=False,
    )
```
